32 devices in a mesh: gx: 8 (over z, y), gy: 4 (over x, core).
Axes of the slice: x: 2, y: 2, z: 4, core: 2. Of those that a mesh axis runs over, the one named last changes fastest.
Arguments:
- velocity_u: float32 [4, 1280, 1024], P(None, 'gy', 'gx'), may hold values from -6 to 6
- velocity_v: float32 [4, 1280, 1024], P(None, 'gy', 'gx'), may hold values from -6 to 6
- tracer: float32 [4, 1280, 1024], P(None, 'gy', 'gx'), may hold values from -6 to 6
- pressure_old: float32 [1280, 1024], P('gy', 'gx'), may hold values from -6 to 6
- depth: float32 [1280, 1024], P('gy', 'gx'), may hold values from 0.5 to 2
- helm: float32 [1280, 1024], P('gy', 'gx'), may hold values from 0.05 to 0.5
- land_mask: int32 [1280, 1024], P('gy', 'gx'), may hold values from 0 to 1, as said below
- clinic_map: int32 [32, 8], replicated, may hold values from 0 to 1, as said below
- tropic_map: int32 [32, 8], replicated, may hold values from -1 to 47, as said below
Outputs:
- velocity_u_new: float32 [4, 1280, 1024], P(None, 'gy', 'gx')
- velocity_v_new: float32 [4, 1280, 1024], P(None, 'gy', 'gx')
- tracer_new: float32 [4, 1280, 1024], P(None, 'gy', 'gx')
- pressure: float32 [1280, 1024], P('gy', 'gx')
The draws below stay inside these ranges and needn't reach their ends.
Inputs may be any that keep to these rules, and one draw needn't show every extreme that they name: `land_mask`: rows 0 and 1279 are land; every column of a block whose tropic_map entry is -1 is land; every other block has an ocean column. `clinic_map`: 1 exactly on the blocks whose tropic_map entry is not -1. `tropic_map`: A quarter of the blocks of every device's clinic domain are -1. Another value t places the block in slot t % 6 of the device with gx index t // 6 and the gy index of the device that holds the block's rows; no slot is named twice. The blocks of one device's clinic domain place at most 1 block on any one device, and this bound is reached; every device receives at most 6 blocks, and this bound is reached.
All inputs are finite; a program needn't handle non-finite values.
Results may differ from the reference program's by a relative error of at most 0.00026.
Values sent between devices are 32-bit elements; how exact they have to be, the bound alone decides.
No kernel may reach another device: no remote copies, remote signals or barrier semaphores. Data moves between devices by JAX's collectives and lax.ppermute only.
A program may use at most 64 MiB of HBM per device.

```python
import math
import jax
import jax.numpy as jnp

KZ = 4
BX = 128
BY = 40
ITERS = 4
NX = 1024
NY = 1280
BPX = 1
BPY = 8
NSUB = 8
KEEP = 6
CAP = 1
NBX = 8
NBY = 32


def block_plan(key):
    base = jax.random.fold_in(key, 4242)
    key_order = jax.random.fold_in(base, 1)
    key_shift = jax.random.fold_in(base, 2)
    key_slots = jax.random.fold_in(base, 3)
    bands = NBY // BPY
    columns = NBX // BPX
    local = jnp.arange(NSUB)
    scores = jax.random.randint(key_order, (bands, columns, NSUB), 0, 1 << 20) * NSUB + local
    order = jnp.argsort(scores, axis=-1)
    ranking = jnp.argsort(order, axis=-1)
    kept = ranking < KEEP
    offset = ranking // CAP
    within = ranking % CAP
    shift = jax.random.randint(key_shift, (bands, 1, 1), 0, columns)
    source = jnp.arange(columns).reshape(1, columns, 1)
    target = (source + shift + offset) % columns
    slot = jnp.where(kept, offset * CAP + within, 0)
    slot_scores = jax.random.randint(key_slots, (bands, columns, KEEP), 0, 1 << 20) * KEEP + jnp.arange(KEEP)
    shuffle = jnp.argsort(slot_scores, axis=-1)
    band_index = jnp.broadcast_to(jnp.arange(bands).reshape(bands, 1, 1), target.shape)
    placed = shuffle[band_index, target, slot]
    value = jnp.where(kept, target * KEEP + placed, -1)
    return value.reshape(bands, columns, BPY, BPX).transpose(0, 2, 1, 3).reshape(NBY, NBX).astype(jnp.int32)


def draw_tropic_map(key, part):
    return block_plan(key)


def draw_clinic_map(key, part):
    return (block_plan(key) >= 0).astype(jnp.int32)


def draw_land_mask(key, part):
    plan = block_plan(key)
    kept = jnp.repeat(jnp.repeat(plan >= 0, BY, axis=0), BX, axis=1)
    landed = jax.random.randint(jax.random.fold_in(key, 99), (NY, NX), 0, 100) < 15
    rows = jnp.arange(NY).reshape(NY, 1)
    cols = jnp.arange(NX).reshape(1, NX)
    centre = (rows % BY == BY // 2) & (cols % BX == BX // 2)
    ocean = kept & (jnp.logical_not(landed) | centre)
    border = (rows == 0) | (rows == NY - 1)
    ocean = ocean & jnp.logical_not(border)
    return ocean.astype(jnp.int32)


def block_levels(own_key, extent, shards, least, high):
    factor_of, own = 1.0, jax.random.fold_in(own_key, 6)
    for dim, shards_of in shards:
        steps = jnp.exp(jax.random.uniform(jax.random.fold_in(own, dim), (shards_of,), jnp.float32, least / len(shards), high / len(shards)))
        factor_of = factor_of * jnp.repeat(steps, extent[dim] // shards_of).reshape([-1 if axis == dim else 1 for axis in range(len(extent))])
    return factor_of


def centred(own_key, extent, scale, most, pieces=(), held_as=jnp.bfloat16):
    factor_of = block_levels(own_key, extent, pieces, -0.22, 0.18) if pieces else 1.0
    drawn = jax.random.normal(own_key, extent, jnp.float32) * scale * factor_of
    return jnp.minimum(jnp.maximum(drawn, -most), most).astype(held_as)


def setup_inputs(seed: int = 0) -> dict:
    streams_of = jax.random.split(jax.random.key(seed), 10)
    velocity_u = centred(streams_of[0], (KZ, NY, NX), 1.0, 6.0, ((1, 4), (2, 8)), jnp.float32)
    velocity_v = centred(streams_of[1], (KZ, NY, NX), 1.0, 6.0, ((1, 4), (2, 8)), jnp.float32)
    tracer = centred(streams_of[2], (KZ, NY, NX), 1.0, 6.0, ((1, 4), (2, 8)), jnp.float32)
    pressure_old = centred(streams_of[3], (NY, NX), 1.0, 6.0, ((0, 4), (1, 8)), jnp.float32)
    depth = jnp.clip(jnp.exp(math.log(2.0) - 1.3862944 * jax.random.uniform(streams_of[4], (NY, NX), jnp.float32) ** block_levels(streams_of[4], (NY, NX), ((0, 4), (1, 8)), -0.2, 0.2)), 0.5, 2.0)
    helm = jnp.clip(jnp.exp(math.log(0.5) - 2.3025851 * jax.random.uniform(streams_of[5], (NY, NX), jnp.float32) ** block_levels(streams_of[5], (NY, NX), ((0, 4), (1, 8)), -0.2, 0.2)), 0.05, 0.5)
    land_mask = draw_land_mask(jax.random.fold_in(streams_of[9], 71), 0)
    clinic_map = draw_clinic_map(jax.random.fold_in(streams_of[9], 71), 0)
    tropic_map = draw_tropic_map(jax.random.fold_in(streams_of[9], 71), 0)
    return {"velocity_u": velocity_u, "velocity_v": velocity_v, "tracer": tracer, "pressure_old": pressure_old, "depth": depth, "helm": helm, "land_mask": land_mask, "clinic_map": clinic_map, "tropic_map": tropic_map}


def mixing(field):
    diff = field[1:] - field[:-1]
    zero = jnp.zeros_like(field[:1])
    return jnp.concatenate([diff, zero], 0) - jnp.concatenate([zero, diff], 0)


def east(a):
    return jnp.roll(a, -1, axis=-1)


def west(a):
    return jnp.roll(a, 1, axis=-1)


def north(a):
    return jnp.roll(a, -1, axis=-2)


def south(a):
    return jnp.roll(a, 1, axis=-2)


def reference(velocity_u, velocity_v, tracer, pressure_old, depth, helm, land_mask, clinic_map, tropic_map):
    f32 = jnp.float32

    def spread(blocks):
        return jnp.repeat(jnp.repeat(blocks, BY, axis=0), BX, axis=1)

    ocean = land_mask.astype(f32)
    domain = spread((tropic_map >= 0).astype(f32))
    active = spread(clinic_map.astype(f32))
    solve_mask = ocean * domain
    wet = depth * solve_mask
    face_e = jnp.minimum(wet, east(wet))
    face_w = jnp.minimum(wet, west(wet))
    face_n = jnp.minimum(wet, north(wet))
    face_s = jnp.minimum(wet, south(wet))

    def diffuse(a):
        return face_e * (east(a) - a) + face_w * (west(a) - a) + face_n * (north(a) - a) + face_s * (south(a) - a)

    latitude = jnp.arange(NY).astype(f32)
    coriolis = (0.2 + 0.6 * ((latitude + 0.5) / NY)).reshape(NY, 1)
    u_star = velocity_u + 0.2 * (0.5 * mixing(velocity_u) + 0.5 * diffuse(velocity_u) + coriolis * velocity_v)
    v_star = velocity_v + 0.2 * (0.5 * mixing(velocity_v) + 0.5 * diffuse(velocity_v) - coriolis * velocity_u)
    tracer_raw = tracer + 0.2 * (0.5 * mixing(tracer) + 0.5 * diffuse(tracer)
                                 - 0.5 * (velocity_u * (east(tracer) - west(tracer)) + velocity_v * (north(tracer) - south(tracer))))
    thick = ((2 * jnp.arange(KZ) + 1).astype(f32) / (KZ * KZ)).reshape(KZ, 1, 1)
    east_flow = wet * jnp.sum(thick * u_star, 0)
    north_flow = wet * jnp.sum(thick * v_star, 0)
    forcing = solve_mask * (-(east_flow - west(east_flow)) - (north_flow - south(north_flow)))
    diagonal = helm + face_e + face_w + face_n + face_s

    def operate(x):
        return diagonal * x - face_e * east(x) - face_w * west(x) - face_n * north(x) - face_s * south(x)

    solution = solve_mask * pressure_old
    residual = forcing - operate(solution)
    precond = residual / diagonal
    direction = precond
    rz_now = jnp.sum(residual * precond)
    for step in range(ITERS):
        image = operate(direction)
        alpha = rz_now / jnp.sum(direction * image)
        solution = solution + alpha * direction
        residual = residual - alpha * image
        if step + 1 < ITERS:
            precond = residual / diagonal
            rz_next = jnp.sum(residual * precond)
            direction = precond + (rz_next / rz_now) * direction
            rz_now = rz_next
    grad_x = east(solution) - solution
    grad_y = north(solution) - solution
    keep = active * ocean
    u_new = keep * (u_star - 1.0 * grad_x) + (1.0 - active) * velocity_u
    v_new = keep * (v_star - 1.0 * grad_y) + (1.0 - active) * velocity_v
    t_new = keep * tracer_raw + (1.0 - active) * tracer
    return u_new, v_new, t_new, solution
```

```python
import jax
import jax.numpy as jnp
from jax import lax
from jax.experimental import pallas as pl
from jax.experimental.pallas import tpu as pltpu
from jax.sharding import PartitionSpec as P

BX = 128
BY = 40
ITERS = 4

step_time = 0.2
viscosity = 0.5
diffusivity = 0.5
vertical = 0.5
gravity = 1.0

SUB = 8
LANES = 128
HALF = LANES // 2
PLANES = ("U", "G", "V", "H", "wet", "start", "helm")
WIDTHS = (ITERS + 2, ITERS + 1, ITERS + 1, ITERS, ITERS + 2, ITERS + 1, ITERS)
OFFSETS = tuple(sum(WIDTHS[:i]) for i in range(len(WIDTHS)))
EDGE = sum(WIDTHS)
NP = len(PLANES)
f32 = jnp.float32


def roll(x, shift, axis=1):
    shift = shift % x.shape[axis]
    return x if shift == 0 else pltpu.roll(x, shift, axis)


def lane_of(x):
    return lax.broadcasted_iota(jnp.int32, x.shape, 1)


def thickness(levels):
    return [(2 * k + 1) / (levels * levels) for k in range(levels)]


def mixed_weights(levels):
    thick = thickness(levels)
    out = list(thick)
    for k in range(levels - 1):
        move = step_time * vertical * (thick[k] - thick[k + 1])
        out[k + 1] += move
        out[k] -= move
    return out


def weighted(weights, fields):
    total = weights[0] * fields[0]
    for w, f in zip(weights[1:], fields[1:]):
        total = total + w * f
    return total


def planes_of(us, vs, pressure_old, depth, helm, land, domain, first_row, total_rows):
    levels = len(us)
    thick, mixed = thickness(levels), mixed_weights(levels)
    row = first_row + lax.broadcasted_iota(jnp.int32, us[0].shape, 0)
    coriolis = 0.2 + 0.6 * ((row.astype(f32) + 0.5) / total_rows)
    u_sum, v_sum = weighted(thick, us), weighted(thick, vs)
    east = weighted(mixed, us) + step_time * coriolis * v_sum
    north = weighted(mixed, vs) - step_time * coriolis * u_sum
    mask = land.astype(f32) * domain
    return (u_sum, east, v_sum, north, depth * mask, mask * pressure_old, helm)


def place():
    return lax.axis_index("gx"), lax.axis_index("gy")


def domain_at(tropic_ref, row_dev, col_dev, rows, row):
    block = row_dev * (rows // BY) + row // BY
    return jnp.where(tropic_ref[block, col_dev] >= 0, 1.0, 0.0).astype(f32)


def rim_kernel(
    rows, total_rows, u, v, t, p, depth, helm, land, tropic, low_out, high_out, s3, s2, si, sems
):
    col_dev, row_dev = place()
    levels = u.shape[0]
    copies = []
    for side, r0 in enumerate((0, rows - SUB)):
        for i, ref in enumerate((u, v, t)):
            copies.append((ref.at[:, pl.ds(r0, SUB), :], s3.at[side, i]))
        for i, ref in enumerate((p, depth, helm)):
            copies.append((ref.at[pl.ds(r0, SUB), :], s2.at[side, i]))
        copies.append((land.at[pl.ds(r0, SUB), :], si.at[side]))
    copies = [pltpu.make_async_copy(a, b, sems.at[i]) for i, (a, b) in enumerate(copies)]
    for c in copies:
        c.start()
    for c in copies:
        c.wait()
    for side, (r0, out) in enumerate(((0, low_out), (rows - SUB, high_out))):
        domain = domain_at(tropic, row_dev, col_dev, rows, r0)
        us = [s3[side, 0, k] for k in range(levels)]
        vs = [s3[side, 1, k] for k in range(levels)]
        planes = planes_of(
            us, vs, s2[side, 0], s2[side, 1], s2[side, 2], si[side], domain,
            row_dev * rows + r0, total_rows,
        )
        for i, plane in enumerate(planes):
            out[pl.ds(SUB * i, SUB), :] = plane
        edge = 0 if side == 0 else SUB - 1
        for i in range(3):
            for k in range(levels):
                n = SUB * NP + i * levels + k
                out[n : n + 1, :] = s3[side, i, k, edge : edge + 1, :]
        used = SUB * NP + 3 * levels
        if used < out.shape[0]:
            out[used:, :] = jnp.zeros((out.shape[0] - used, LANES), f32)


def pack_pair(low_fields, high_fields, extra_low, extra_high, to_west):
    shape = low_fields[0].shape
    lane = lax.broadcasted_iota(jnp.int32, shape, 1)
    out = jnp.zeros(shape, f32)
    for base, fields, extra in ((0, low_fields, extra_low), (HALF, high_fields, extra_high)):
        for f, w, off in zip(fields, WIDTHS, OFFSETS):
            lo = base + off
            first = 0 if to_west else LANES - w
            out = jnp.where((lane >= lo) & (lane < lo + w), roll(f, lo - first), out)
        for i, f in enumerate(extra):
            lo = base + EDGE + i
            first = 0 if to_west else LANES - 1
            out = jnp.where(lane == lo, roll(f, lo - first), out)
    return out


def plane_kernel(rows, total_rows, u, v, t, p, depth, helm, land, tropic, planes, west, east):
    col_dev, row_dev = place()
    levels = u.shape[0]
    half = rows // 2

    def at(r):
        r = pl.multiple_of(r, SUB)
        here = pl.ds(r, SUB)
        us = [u[k, here, :] for k in range(levels)]
        vs = [v[k, here, :] for k in range(levels)]
        ts = [t[k, here, :] for k in range(levels)]
        domain = domain_at(tropic, row_dev, col_dev, rows, r)
        out = planes_of(
            us, vs, p[here, :], depth[here, :], helm[here, :], land[here, :], domain,
            row_dev * rows + r, total_rows,
        )
        for i, plane in enumerate(out):
            planes[i, here, :] = plane
        return out, us + vs + ts

    unroll = 4

    def body(i, carry):
        for j in range(unroll):
            r = (i * unroll + j) * SUB
            low, extra_low = at(r)
            high, extra_high = at(r + half)
            here = pl.ds(pl.multiple_of(r, SUB), SUB)
            west[here, :] = pack_pair(low, high, extra_low, extra_high, True)
            east[here, :] = pack_pair(low, high, extra_low, extra_high, False)
        return carry

    lax.fori_loop(0, half // (SUB * unroll), body, 0)


def corner_kernel(from_low, from_high, west_in, east_in, west, east):
    low = [from_low[pl.ds(SUB * i, SUB), :] for i in range(NP)]
    high = [from_high[pl.ds(SUB * i, SUB), :] for i in range(NP)]
    west[...] = pack_pair(low, high, [], [], True)
    east[...] = pack_pair(low, high, [], [], False)


def shifted(c, h):
    lane = lane_of(c)
    rc, rh = roll(c, -1), roll(h, -1)
    last = lane == LANES - 1
    east = jnp.where(last, rh, rc), jnp.where(last, rc, rh)
    rc, rh = roll(c, 1), roll(h, 1)
    first = lane == 0
    west = jnp.where(first, rh, rc), jnp.where(first, rc, rh)
    return east, west


CH = 24


def solve_kernel(
    rows, planes, from_low, from_high, from_west, from_east,
    basis, faces, partial, F, face_e, face_n, flow_e, flow_n, T, coef, diag,
):
    ext = rows + 2 * SUB
    half = rows // 2
    top = ext + SUB
    zero8 = jnp.zeros((SUB, LANES), f32)
    for c in range(2):
        for r in (0, top):
            for i in range(NP):
                F[i, c, pl.ds(r, SUB), :] = zero8
            face_e[c, pl.ds(r, SUB), :] = zero8
            face_n[c, pl.ds(r, SUB), :] = zero8
            flow_n[c, pl.ds(r, SUB), :] = zero8
            for k in range(ITERS):
                T[k, c, pl.ds(r, SUB), :] = zero8

    def unpack(dst, src, base):
        e, w = from_east[src, :], from_west[src, :]
        lane = lane_of(e)
        for i in range(NP):
            lo = base + OFFSETS[i]
            width = WIDTHS[i]
            he = roll(e, -lo)
            hw = roll(w, LANES - width - lo)
            h = jnp.where(lane < width, he, jnp.where(lane >= LANES - width, hw, 0.0))
            F[i, 1, dst, :] = h

    for i in range(NP):
        F[i, 0, pl.ds(SUB, SUB), :] = from_low[pl.ds(SUB * i, SUB), :]
        F[i, 0, pl.ds(SUB + SUB + rows, SUB), :] = from_high[pl.ds(SUB * i, SUB), :]
        F[i, 0, pl.ds(2 * SUB, rows), :] = planes[i]
    unpack(pl.ds(SUB, SUB), pl.ds(half, SUB), 0)
    unpack(pl.ds(2 * SUB + rows, SUB), pl.ds(half, SUB), HALF)
    step = 40
    for r in range(0, half, step):
        unpack(pl.ds(2 * SUB + r, step), pl.ds(r, step), 0)
        unpack(pl.ds(2 * SUB + half + r, step), pl.ds(r, step), HALF)

    iU, iG, iV, iH, iW, iS, iM = range(NP)
    chunks = [(SUB + r) for r in range(0, ext, CH)]
    assert ext % CH == 0
    both = (0, 1)

    def load(ref, idx, r, d=0):
        return tuple(ref[idx + (c, slice(r + d, r + d + CH), slice(None))] for c in both)

    def store(ref, idx, r, value):
        for c in both:
            ref[idx + (c, slice(r, r + CH), slice(None))] = value[c]

    def around(ref, idx, r):
        x = load(ref, idx, r)
        e, w = shifted(*x)
        return x, e, w, load(ref, idx, r, 1), load(ref, idx, r, -1)

    def stage_faces(r):
        x, e, _, n, _ = around(F, (iW,), r)
        store(face_e, (), r, tuple(jnp.minimum(x[c], e[c]) for c in both))
        store(face_n, (), r, tuple(jnp.minimum(x[c], n[c]) for c in both))

    def stage_flows(r):
        fe, fn, fs = load(face_e, (), r), load(face_n, (), r), load(face_n, (), r, -1)
        _, fw = shifted(*fe)
        wet = load(F, (iW,), r)
        for field, base, out in ((iU, iG, flow_e), (iV, iH, flow_n)):
            x, e, w, n, s = around(F, (field,), r)
            g = load(F, (base,), r)
            flow = []
            for c in both:
                d = (
                    fe[c] * (e[c] - x[c]) + fw[c] * (w[c] - x[c])
                    + fn[c] * (n[c] - x[c]) + fs[c] * (s[c] - x[c])
                )
                flow.append(wet[c] * (g[c] + (step_time * viscosity) * d))
            store(out, (), r, flow)

    def core_rows(r):
        lo, hi = max(r, 2 * SUB), min(r + CH, 2 * SUB + rows)
        return lo - r, hi - r

    sums = [None] * (2 * ITERS)

    def add_sum(i, r, value):
        lo, hi = core_rows(r)
        for q in range(lo, hi, SUB):
            part = value[q : q + SUB]
            sums[i] = part if sums[i] is None else sums[i] + part

    def stage_residual(r):
        fe, fn, fs = load(face_e, (), r), load(face_n, (), r), load(face_n, (), r, -1)
        _, fw = shifted(*fe)
        wet, helm = load(F, (iW,), r), load(F, (iM,), r)
        ef = load(flow_e, (), r)
        _, efw = shifted(*ef)
        nf, nfs = load(flow_n, (), r), load(flow_n, (), r, -1)
        x, e, w, n, s = around(F, (iS,), r)
        lo, hi = core_rows(r)
        for c in both:
            mask = wet[c] > 0.0
            force = jnp.where(mask, -(ef[c] - efw[c]) - (nf[c] - nfs[c]), 0.0)
            d = helm[c] + fe[c] + fw[c] + fn[c] + fs[c]
            res = force - (
                d * x[c] - fe[c] * e[c] - fw[c] * w[c] - fn[c] * n[c] - fs[c] * s[c]
            )
            inv = 1.0 / jnp.where(d > 0.0, d, 1.0)
            z = res * inv
            here = slice(r, r + CH)
            T[0, c, here, :] = z
            for i, f in enumerate((fe, fw, fn, fs)):
                coef[i, c, here, :] = f[c] * inv
            if c == 0:
                diag[here, :] = d
                add_sum(0, r, res * z)
                for i, f in enumerate((fe, fw, fn, fs)):
                    faces[i, r + lo - 2 * SUB : r + hi - 2 * SUB, :] = f[0][lo:hi]

    def stage_step(k, r):
        x, e, w, n, s = around(T, (k,), r)
        here = slice(r, r + CH)
        for c in both if k + 1 < ITERS else (0,):
            y = (
                coef[0, c, here, :] * e[c] + coef[1, c, here, :] * w[c]
                + coef[2, c, here, :] * n[c] + coef[3, c, here, :] * s[c]
            )
            if k > 0:
                y = 2.0 * y - T[k - 1, c, here, :]
            if k + 1 < ITERS:
                T[k + 1, c, here, :] = y
            if c == 0:
                d = diag[here, :]
                add_sum(2 * k + 1, r, d * x[c] * y)
                if k + 1 < ITERS:
                    add_sum(2 * k + 2, r, d * y * y)

    stages = [stage_faces, stage_flows, stage_residual]
    stages += [lambda r, k=k: stage_step(k, r) for k in range(ITERS)]
    lags = [0]
    for _ in stages[1:]:
        lags.append(lags[-1] + 1)
    lags = [0, 1, 2] + [2 + 2 * (k + 1) for k in range(ITERS)]
    for i in range(len(chunks) + lags[-1]):
        for stage, lag in zip(stages, lags):
            if 0 <= i - lag < len(chunks):
                stage(chunks[i - lag])

    for c in both:
        basis[0, c] = F[iS, c, SUB : SUB + ext, :]
        for k in range(ITERS):
            basis[k + 1, c] = T[k, c, SUB : SUB + ext, :]
    lane = lax.broadcasted_iota(jnp.int32, (1, LANES), 1)
    line = jnp.zeros((1, LANES), f32)
    for i, total in enumerate(sums):
        one = jnp.sum(jnp.sum(total, axis=0, keepdims=True), axis=1, keepdims=True)
        line = jnp.where(lane == i, one, line)
    partial[...] = jnp.broadcast_to(line, partial.shape)


def coefficients(m):
    n = ITERS

    def gram(i, j):
        return 0.5 * (m[i + j] + m[abs(i - j)])

    G = [[gram(i, j) for j in range(n)] for i in range(n)]
    H = [[gram(i, j) - 0.5 * (gram(i, j + 1) + gram(i, abs(j - 1))) for j in range(n)] for i in range(n)]
    zero = jnp.zeros_like(m[0])

    def quad(a, Q):
        total = zero
        for i in range(len(a)):
            total = total + a[i] * a[i] * Q[i][i]
            for j in range(i):
                total = total + 2.0 * a[i] * a[j] * Q[i][j]
        return total

    def ratio(a, b):
        return jnp.where(b > 0.0, a / jnp.where(b > 0.0, b, 1.0), 0.0)

    z = [jnp.ones_like(zero)]
    p = list(z)
    x = [zero] * n
    rz = m[0]
    for it in range(n):
        alpha = ratio(rz, quad(p, H))
        for i in range(len(p)):
            x[i] = x[i] + alpha * p[i]
        if it + 1 == n:
            break
        image = p + [zero]
        for j in range(len(p)):
            if j == 0:
                image[1] = image[1] - p[0]
            else:
                image[j + 1] = image[j + 1] - 0.5 * p[j]
                image[j - 1] = image[j - 1] - 0.5 * p[j]
        z = [a - alpha * b for a, b in zip(z + [zero], image)]
        rz_next = quad(z, G)
        beta = ratio(rz_next, rz)
        p = [a + beta * b for a, b in zip(z, p + [zero])]
        rz = rz_next
    return x


def finish_kernel(
    rows, total_rows, u, v, t, land, clinic, parts, basis, faces, from_low, from_high, from_west,
    from_east, u_out, v_out, t_out, p_out, pres,
):
    col_dev, row_dev = place()
    levels = u.shape[0]
    half = rows // 2
    lane1 = lax.broadcasted_iota(jnp.int32, (1, LANES), 1)
    line = jnp.sum(parts[...], axis=0, keepdims=True)
    sums = []
    for i in range(2 * ITERS):
        one = jnp.sum(jnp.where(lane1 == i, line, 0.0), axis=1, keepdims=True)
        sums.append(jnp.broadcast_to(one, (1, LANES)))
    m = sums[:2] + [2.0 * s - sums[i % 2] for i, s in enumerate(sums[2:])]
    x = coefficients(m)
    ext = rows + 2 * SUB
    for r in range(0, ext, CH):
        here = slice(r, r + CH)
        for c in range(2):
            total = basis[0, c, here, :]
            for k in range(ITERS):
                total = total + x[k] * basis[k + 1, c, here, :]
            pres[c, here, :] = total

    for r in range(0, rows, BY):
        block = row_dev * (rows // BY) + r // BY
        active = clinic[block, col_dev].astype(f32)
        here = pl.ds(r, BY)
        keep = land[here, :].astype(f32) * active
        rest = 1.0 - active
        pc = pres[0, SUB + r : SUB + r + BY, :]
        ph = pres[1, SUB + r : SUB + r + BY, :]
        p_out[here, :] = pc
        lane = lane_of(pc)
        first, last = lane == 0, lane == LANES - 1
        grad_x = jnp.where(last, roll(ph, -1), roll(pc, -1)) - pc
        grad_y = pres[0, SUB + r + 1 : SUB + r + BY + 1, :] - pc
        fe, fw, fn, fs = (faces[i, here, :] for i in range(4))
        row = row_dev * rows + r + lax.broadcasted_iota(jnp.int32, (BY, LANES), 0)
        coriolis = 0.2 + 0.6 * ((row.astype(f32) + 0.5) / total_rows)
        src = pl.ds(r % half, BY)
        base = HALF * (r // half) + EDGE

        def around(ref, which, k):
            n_row = SUB * NP + which * levels + k
            a = ref[k, here, :]
            lo = base + which * levels + k
            e = jnp.where(last, roll(from_east[src, :], LANES - 1 - lo), roll(a, -1))
            w = jnp.where(first, roll(from_west[src, :], -lo), roll(a, 1))
            if r + BY < rows:
                n = ref[k, r + 1 : r + BY + 1, :]
            else:
                n = jnp.concatenate([a[1:], from_high[n_row : n_row + 1, :]], 0)
            if r > 0:
                s = ref[k, r - 1 : r + BY - 1, :]
            else:
                s = jnp.concatenate([from_low[n_row : n_row + 1, :], a[:-1]], 0)
            return a, e, w, n, s

        def diffuse(a, e, w, n, s):
            return fe * (e - a) + fw * (w - a) + fn * (n - a) + fs * (s - a)

        def mixing(ref, k, a):
            total = None
            if k + 1 < levels:
                total = ref[k + 1, here, :] - a
            if k > 0:
                down = a - ref[k - 1, here, :]
                total = -down if total is None else total - down
            return jnp.zeros_like(a) if total is None else total

        for k in range(levels):
            ua = around(u, 0, k)
            va = around(v, 1, k)
            ta = around(t, 2, k)
            uc, vc, tc = ua[0], va[0], ta[0]
            u_star = uc + step_time * (
                vertical * mixing(u, k, uc) + viscosity * diffuse(*ua) + coriolis * vc
            )
            v_star = vc + step_time * (
                vertical * mixing(v, k, vc) + viscosity * diffuse(*va) - coriolis * uc
            )
            raw = tc + step_time * (
                vertical * mixing(t, k, tc) + diffusivity * diffuse(*ta)
                - 0.5 * (uc * (ta[1] - ta[2]) + vc * (ta[3] - ta[4]))
            )
            u_out[k, here, :] = keep * (u_star - gravity * grad_x) + rest * uc
            v_out[k, here, :] = keep * (v_star - gravity * grad_y) + rest * vc
            t_out[k, here, :] = keep * raw + rest * tc


VMEM = pl.BlockSpec(memory_space=pltpu.VMEM)
SMEM = pl.BlockSpec(memory_space=pltpu.SMEM)
ANY = pl.BlockSpec(memory_space=pl.ANY)


def shape(*dims):
    return jax.ShapeDtypeStruct(dims, f32)


def on_device(
    velocity_u, velocity_v, tracer, pressure_old, depth, helm, land_mask, clinic_map, tropic_map
):
    levels, rows, cols = velocity_u.shape
    nx, ny = lax.axis_size("gx"), lax.axis_size("gy")
    total_rows = rows * ny
    assert cols == LANES == BX and rows % BY == 0 and rows % (2 * BY) == 0
    assert EDGE + 3 * levels <= HALF and ITERS + 2 <= SUB
    half = rows // 2
    ext = rows + 2 * SUB
    strip = -(-(SUB * NP + 3 * levels) // SUB) * SUB
    fields = (velocity_u, velocity_v, tracer, pressure_old, depth, helm, land_mask, tropic_map)

    def params(**kw):
        return pltpu.CompilerParams(vmem_limit_bytes=40 << 20, **kw)

    low, high = pl.pallas_call(
        lambda *a: rim_kernel(rows, total_rows, *a),
        out_shape=(shape(strip, LANES), shape(strip, LANES)),
        in_specs=[ANY] * 7 + [SMEM],
        out_specs=(VMEM, VMEM),
        scratch_shapes=[
            pltpu.VMEM((2, 3, levels, SUB, LANES), f32),
            pltpu.VMEM((2, 3, SUB, LANES), f32),
            pltpu.VMEM((2, SUB, LANES), jnp.int32),
            pltpu.SemaphoreType.DMA((14,)),
        ],
        name="rim",
    )(*fields)
    up = [(i, (i + 1) % ny) for i in range(ny)]
    down = [((i + 1) % ny, i) for i in range(ny)]
    from_low = lax.ppermute(high, "gy", up)
    from_high = lax.ppermute(low, "gy", down)
    planes, west, east = pl.pallas_call(
        lambda *a: plane_kernel(rows, total_rows, *a),
        out_shape=(
            shape(NP, rows, LANES), shape(half + SUB, LANES), shape(half + SUB, LANES),
        ),
        in_specs=[VMEM] * 7 + [SMEM],
        out_specs=(VMEM, VMEM, VMEM),
        compiler_params=params(),
        name="planes",
    )(*fields)
    strip_spec = pl.BlockSpec((strip, LANES), lambda i: (0, 0))
    corner = pl.BlockSpec((SUB, LANES), lambda i: (half // SUB, 0))
    west, east = pl.pallas_call(
        corner_kernel,
        grid=(1,),
        out_shape=(shape(half + SUB, LANES),) * 2,
        in_specs=[strip_spec, strip_spec, ANY, ANY],
        out_specs=(corner, corner),
        input_output_aliases={2: 0, 3: 1},
        name="corners",
    )(from_low, from_high, west, east)
    right = [(i, (i + 1) % nx) for i in range(nx)]
    left = [((i + 1) % nx, i) for i in range(nx)]
    from_west = lax.ppermute(east, "gx", right)
    from_east = lax.ppermute(west, "gx", left)
    tall = ext + 2 * SUB
    basis, faces, partial = pl.pallas_call(
        lambda *a: solve_kernel(rows, *a),
        out_shape=(
            shape(ITERS + 1, 2, ext, LANES), shape(4, rows, LANES), shape(nx * ny, LANES),
        ),
        in_specs=[VMEM] * 5,
        out_specs=(VMEM, VMEM, VMEM),
        scratch_shapes=[
            pltpu.VMEM((NP, 2, tall, LANES), f32),
            pltpu.VMEM((2, tall, LANES), f32),
            pltpu.VMEM((2, tall, LANES), f32),
            pltpu.VMEM((2, tall, LANES), f32),
            pltpu.VMEM((2, tall, LANES), f32),
            pltpu.VMEM((ITERS, 2, tall, LANES), f32),
            pltpu.VMEM((4, 2, tall, LANES), f32),
            pltpu.VMEM((tall, LANES), f32),
        ],
        compiler_params=params(),
        name="solve",
    )(planes, from_low, from_high, from_west, from_east)
    parts = lax.all_to_all(partial, ("gx", "gy"), 0, 0, tiled=True)
    return pl.pallas_call(
        lambda *a: finish_kernel(rows, total_rows, *a),
        out_shape=(shape(levels, rows, LANES),) * 3 + (shape(rows, LANES),),
        in_specs=[VMEM] * 4 + [SMEM] + [VMEM] * 7,
        out_specs=(VMEM,) * 4,
        scratch_shapes=[pltpu.VMEM((2, ext, LANES), f32)],
        compiler_params=params(),
        name="finish",
    )(
        velocity_u, velocity_v, tracer, land_mask, clinic_map, parts, basis, faces, from_low,
        from_high, from_west, from_east,
    )


def solution(mesh):
    in_specs = (
        P(None, "gy", "gx"),
        P(None, "gy", "gx"),
        P(None, "gy", "gx"),
        P("gy", "gx"),
        P("gy", "gx"),
        P("gy", "gx"),
        P("gy", "gx"),
        P(),
        P(),
    )
    out_specs = (P(None, "gy", "gx"), P(None, "gy", "gx"), P(None, "gy", "gx"), P("gy", "gx"))
    return jax.shard_map(
        on_device, mesh=mesh, in_specs=in_specs, out_specs=out_specs, check_vma=False
    )
```

```python
import jax
import jax.numpy as jnp
from jax import lax
from jax.experimental import pallas as pl
from jax.experimental.pallas import tpu as pltpu
from jax.sharding import PartitionSpec as P

BX = 128
BY = 40
ITERS = 4

step_time = 0.2
viscosity = 0.5
diffusivity = 0.5
vertical = 0.5
gravity = 1.0

SUB = 8
LANES = 128
HALF = LANES // 2
PLANES = ("U", "G", "V", "H", "wet", "start", "helm")
WIDTHS = (ITERS + 2, ITERS + 1, ITERS + 1, ITERS, ITERS + 2, ITERS + 1, ITERS)
OFFSETS = tuple(sum(WIDTHS[:i]) for i in range(len(WIDTHS)))
EDGE = sum(WIDTHS)
NP = len(PLANES)
WET = PLANES.index("wet")
OTHERS = tuple(i for i in range(NP) if i != WET)
f32 = jnp.float32


def roll(x, shift, axis=1):
    shift = shift % x.shape[axis]
    return x if shift == 0 else pltpu.roll(x, shift, axis)


def lane_of(x):
    return lax.broadcasted_iota(jnp.int32, x.shape, 1)


def thickness(levels):
    return [(2 * k + 1) / (levels * levels) for k in range(levels)]


def mixed_weights(levels):
    thick = thickness(levels)
    out = list(thick)
    for k in range(levels - 1):
        move = step_time * vertical * (thick[k] - thick[k + 1])
        out[k + 1] += move
        out[k] -= move
    return out


def weighted(weights, fields):
    total = weights[0] * fields[0]
    for w, f in zip(weights[1:], fields[1:]):
        total = total + w * f
    return total


def planes_of(us, vs, pressure_old, depth, helm, land, domain, first_row, total_rows):
    levels = len(us)
    thick, mixed = thickness(levels), mixed_weights(levels)
    row = first_row + lax.broadcasted_iota(jnp.int32, us[0].shape, 0)
    coriolis = 0.2 + 0.6 * ((row.astype(f32) + 0.5) / total_rows)
    u_sum, v_sum = weighted(thick, us), weighted(thick, vs)
    east = weighted(mixed, us) + step_time * coriolis * v_sum
    north = weighted(mixed, vs) - step_time * coriolis * u_sum
    mask = land.astype(f32) * domain
    return (u_sum, east, v_sum, north, depth * mask, mask * pressure_old, helm)


def place():
    return lax.axis_index("gx"), lax.axis_index("gy")


def domain_at(tropic_ref, row_dev, col_dev, rows, row):
    block = row_dev * (rows // BY) + row // BY
    return jnp.where(tropic_ref[col_dev, block] >= 0, 1.0, 0.0).astype(f32)


def rim_kernel(
    rows, total_rows, u, v, t, p, depth, helm, land, tropic, low_out, high_out, s3, s2, si, sems
):
    col_dev, row_dev = place()
    levels = u.shape[0]
    copies = []
    for side, r0 in enumerate((0, rows - SUB)):
        for i, ref in enumerate((u, v, t)):
            copies.append((ref.at[:, pl.ds(r0, SUB), :], s3.at[side, i]))
        for i, ref in enumerate((p, depth, helm)):
            copies.append((ref.at[pl.ds(r0, SUB), :], s2.at[side, i]))
        copies.append((land.at[pl.ds(r0, SUB), :], si.at[side]))
    copies = [pltpu.make_async_copy(a, b, sems.at[i]) for i, (a, b) in enumerate(copies)]
    for c in copies:
        c.start()
    for c in copies:
        c.wait()
    for side, (r0, out) in enumerate(((0, low_out), (rows - SUB, high_out))):
        domain = domain_at(tropic, row_dev, col_dev, rows, r0)
        us = [s3[side, 0, k] for k in range(levels)]
        vs = [s3[side, 1, k] for k in range(levels)]
        planes = planes_of(
            us, vs, s2[side, 0], s2[side, 1], s2[side, 2], si[side], domain,
            row_dev * rows + r0, total_rows,
        )
        for i, plane in enumerate(planes):
            out[pl.ds(SUB * i, SUB), :] = plane
        edge = 0 if side == 0 else SUB - 1
        for i in range(3):
            for k in range(levels):
                n = SUB * NP + i * levels + k
                out[n : n + 1, :] = s3[side, i, k, edge : edge + 1, :]
        used = SUB * NP + 3 * levels
        if used < out.shape[0]:
            out[used:, :] = jnp.zeros((out.shape[0] - used, LANES), f32)


def pack_pair(low_fields, high_fields, extra_low, extra_high, to_west):
    shape = low_fields[0].shape
    lane = lax.broadcasted_iota(jnp.int32, shape, 1)
    out = jnp.zeros(shape, f32)
    for base, fields, extra in ((0, low_fields, extra_low), (HALF, high_fields, extra_high)):
        for f, w, off in zip(fields, WIDTHS, OFFSETS):
            lo = base + off
            first = 0 if to_west else LANES - w
            out = jnp.where((lane >= lo) & (lane < lo + w), roll(f, lo - first), out)
        for i, f in enumerate(extra):
            lo = base + EDGE + i
            first = 0 if to_west else LANES - 1
            out = jnp.where(lane == lo, roll(f, lo - first), out)
    return out


def plane_kernel(
    rows, total_rows, u, v, t, p, depth, helm, land, tropic, planes, wet, west, east, u_copy, v_copy
):
    col_dev, row_dev = place()
    levels = u.shape[0]
    half = rows // 2

    def at(r):
        r = pl.multiple_of(r, SUB)
        here = pl.ds(r, SUB)
        us = [u[k, here, :] for k in range(levels)]
        vs = [v[k, here, :] for k in range(levels)]
        ts = [t[k, here, :] for k in range(levels)]
        domain = domain_at(tropic, row_dev, col_dev, rows, r)
        out = planes_of(
            us, vs, p[here, :], depth[here, :], helm[here, :], land[here, :], domain,
            row_dev * rows + r, total_rows,
        )
        for i, plane in zip(OTHERS, range(NP - 1)):
            planes[plane, here, :] = out[i]
        wet[here, :] = out[WET]
        for k in range(levels):
            u_copy[k, here, :] = us[k]
            v_copy[k, here, :] = vs[k]
        return out, us + vs + ts

    unroll = 4

    def body(i, carry):
        for j in range(unroll):
            r = (i * unroll + j) * SUB
            low, extra_low = at(r)
            high, extra_high = at(r + half)
            here = pl.ds(pl.multiple_of(r, SUB), SUB)
            west[here, :] = pack_pair(low, high, extra_low, extra_high, True)
            east[here, :] = pack_pair(low, high, extra_low, extra_high, False)
        return carry

    lax.fori_loop(0, half // (SUB * unroll), body, 0)


def corner_kernel(from_low, from_high, west_in, east_in, west, east):
    low = [from_low[pl.ds(SUB * i, SUB), :] for i in range(NP)]
    high = [from_high[pl.ds(SUB * i, SUB), :] for i in range(NP)]
    west[...] = pack_pair(low, high, [], [], True)
    east[...] = pack_pair(low, high, [], [], False)


def shifted(c, h):
    lane = lane_of(c)
    rc, rh = roll(c, -1), roll(h, -1)
    last = lane == LANES - 1
    east = jnp.where(last, rh, rc), jnp.where(last, rc, rh)
    rc, rh = roll(c, 1), roll(h, 1)
    first = lane == 0
    west = jnp.where(first, rh, rc), jnp.where(first, rc, rh)
    return east, west


CH = 24


def solve_kernel(
    rows, planes, wet_in, from_low, from_high, from_west, from_east,
    basis, edge, partial, F, face_e, face_n, flow_e, flow_n, T, coef, diag,
):
    ext = rows + 2 * SUB
    half = rows // 2
    top = ext + SUB
    zero8 = jnp.zeros((SUB, LANES), f32)
    for c in range(2):
        for r in (0, top):
            for i in range(NP):
                F[i, c, pl.ds(r, SUB), :] = zero8
            face_e[c, pl.ds(r, SUB), :] = zero8
            face_n[c, pl.ds(r, SUB), :] = zero8
            flow_n[c, pl.ds(r, SUB), :] = zero8
            for k in range(ITERS):
                T[k, c, pl.ds(r, SUB), :] = zero8

    def unpack(dst, src, base):
        e, w = from_east[src, :], from_west[src, :]
        lane = lane_of(e)
        for i in range(NP):
            lo = base + OFFSETS[i]
            width = WIDTHS[i]
            he = roll(e, -lo)
            hw = roll(w, LANES - width - lo)
            h = jnp.where(lane < width, he, jnp.where(lane >= LANES - width, hw, 0.0))
            F[i, 1, dst, :] = h

    for i in range(NP):
        F[i, 0, pl.ds(SUB, SUB), :] = from_low[pl.ds(SUB * i, SUB), :]
        F[i, 0, pl.ds(SUB + SUB + rows, SUB), :] = from_high[pl.ds(SUB * i, SUB), :]
        F[i, 0, pl.ds(2 * SUB, rows), :] = wet_in[...] if i == WET else planes[OTHERS.index(i)]
    unpack(pl.ds(SUB, SUB), pl.ds(half, SUB), 0)
    unpack(pl.ds(2 * SUB + rows, SUB), pl.ds(half, SUB), HALF)
    step = 40
    for r in range(0, half, step):
        unpack(pl.ds(2 * SUB + r, step), pl.ds(r, step), 0)
        unpack(pl.ds(2 * SUB + half + r, step), pl.ds(r, step), HALF)

    iU, iG, iV, iH, iW, iS, iM = range(NP)
    chunks = [(SUB + r) for r in range(0, ext, CH)]
    assert ext % CH == 0
    both = (0, 1)

    def load(ref, idx, r, d=0):
        return tuple(ref[idx + (c, slice(r + d, r + d + CH), slice(None))] for c in both)

    def store(ref, idx, r, value):
        for c in both:
            ref[idx + (c, slice(r, r + CH), slice(None))] = value[c]

    def around(ref, idx, r):
        x = load(ref, idx, r)
        e, w = shifted(*x)
        return x, e, w, load(ref, idx, r, 1), load(ref, idx, r, -1)

    def stage_faces(r):
        x, e, _, n, _ = around(F, (iW,), r)
        store(face_e, (), r, tuple(jnp.minimum(x[c], e[c]) for c in both))
        store(face_n, (), r, tuple(jnp.minimum(x[c], n[c]) for c in both))

    def stage_flows(r):
        fe, fn, fs = load(face_e, (), r), load(face_n, (), r), load(face_n, (), r, -1)
        _, fw = shifted(*fe)
        wet = load(F, (iW,), r)
        for field, base, out in ((iU, iG, flow_e), (iV, iH, flow_n)):
            x, e, w, n, s = around(F, (field,), r)
            g = load(F, (base,), r)
            flow = []
            for c in both:
                d = (
                    fe[c] * (e[c] - x[c]) + fw[c] * (w[c] - x[c])
                    + fn[c] * (n[c] - x[c]) + fs[c] * (s[c] - x[c])
                )
                flow.append(wet[c] * (g[c] + (step_time * viscosity) * d))
            store(out, (), r, flow)

    def core_rows(r):
        lo, hi = max(r, 2 * SUB), min(r + CH, 2 * SUB + rows)
        return lo - r, hi - r

    def keep_core(ref, i, r, value):
        lo, hi = core_rows(r)
        ref[i, r + lo - 2 * SUB : r + hi - 2 * SUB, :] = value[lo:hi]

    sums = [None] * (2 * ITERS)

    def add_sum(i, r, value):
        lo, hi = core_rows(r)
        for q in range(lo, hi, SUB):
            part = value[q : q + SUB]
            sums[i] = part if sums[i] is None else sums[i] + part

    def stage_residual(r):
        fe, fn, fs = load(face_e, (), r), load(face_n, (), r), load(face_n, (), r, -1)
        _, fw = shifted(*fe)
        wet, helm = load(F, (iW,), r), load(F, (iM,), r)
        ef = load(flow_e, (), r)
        _, efw = shifted(*ef)
        nf, nfs = load(flow_n, (), r), load(flow_n, (), r, -1)
        x, e, w, n, s = around(F, (iS,), r)
        for c in both:
            mask = wet[c] > 0.0
            force = jnp.where(mask, -(ef[c] - efw[c]) - (nf[c] - nfs[c]), 0.0)
            d = helm[c] + fe[c] + fw[c] + fn[c] + fs[c]
            res = force - (
                d * x[c] - fe[c] * e[c] - fw[c] * w[c] - fn[c] * n[c] - fs[c] * s[c]
            )
            inv = 1.0 / jnp.where(d > 0.0, d, 1.0)
            z = res * inv
            here = slice(r, r + CH)
            T[0, c, here, :] = z
            for i, f in enumerate((fe, fw, fn, fs)):
                coef[i, c, here, :] = f[c] * inv
            if c == 0:
                diag[here, :] = d
                add_sum(0, r, res * z)
                keep_core(basis, 0, r, x[0])
                keep_core(basis, 1, r, z)

    def stage_step(k, r):
        x, e, w, n, s = around(T, (k,), r)
        here = slice(r, r + CH)
        for c in both if k + 1 < ITERS else (0,):
            y = (
                coef[0, c, here, :] * e[c] + coef[1, c, here, :] * w[c]
                + coef[2, c, here, :] * n[c] + coef[3, c, here, :] * s[c]
            )
            if k > 0:
                y = 2.0 * y - T[k - 1, c, here, :]
            if k + 1 < ITERS:
                T[k + 1, c, here, :] = y
            if c == 0:
                d = diag[here, :]
                add_sum(2 * k + 1, r, d * x[c] * y)
                if k + 1 < ITERS:
                    add_sum(2 * k + 2, r, d * y * y)
                    keep_core(basis, k + 2, r, y)

    stages = [stage_faces, stage_flows, stage_residual]
    stages += [lambda r, k=k: stage_step(k, r) for k in range(ITERS)]
    lags = [0]
    for _ in stages[1:]:
        lags.append(lags[-1] + 1)
    lags = [0, 1, 2] + [2 + 2 * (k + 1) for k in range(ITERS)]
    for i in range(len(chunks) + lags[-1]):
        for stage, lag in zip(stages, lags):
            if 0 <= i - lag < len(chunks):
                stage(chunks[i - lag])

    vectors = [lambda c, here: F[iS, c, here, :]]
    vectors += [lambda c, here, k=k: T[k, c, here, :] for k in range(ITERS)]
    assert len(vectors) + 2 <= SUB
    for r in range(0, rows, BY):
        here = slice(2 * SUB + r, 2 * SUB + r + BY)
        side = F[iW, 1, here, :]
        lane = lane_of(side)
        tile = jnp.where(lane == SUB, roll(side, SUB), 0.0)
        tile = jnp.where(lane == SUB + 1, roll(side, SUB + 2), tile)
        for j, get in enumerate(vectors):
            tile = jnp.where(lane == j, roll(get(1, here), j), tile)
        edge[r : r + BY, :] = tile
    north = 2 * SUB + rows
    edge[rows:, :] = jnp.zeros((SUB, LANES), f32)
    for j, get in enumerate(vectors):
        edge[rows + j : rows + j + 1, :] = get(0, slice(north, north + 1))
    edge[rows + SUB - 2 : rows + SUB - 1, :] = F[iW, 0, north : north + 1, :]
    edge[rows + SUB - 1 :, :] = F[iW, 0, 2 * SUB - 1 : 2 * SUB, :]
    lane = lax.broadcasted_iota(jnp.int32, (1, LANES), 1)
    line = jnp.zeros((1, LANES), f32)
    for i, total in enumerate(sums):
        one = jnp.sum(jnp.sum(total, axis=0, keepdims=True), axis=1, keepdims=True)
        line = jnp.where(lane == i, one, line)
    partial[...] = jnp.broadcast_to(line, partial.shape)


def coefficients(m):
    n = ITERS

    def gram(i, j):
        return 0.5 * (m[i + j] + m[abs(i - j)])

    G = [[gram(i, j) for j in range(n)] for i in range(n)]
    H = [[gram(i, j) - 0.5 * (gram(i, j + 1) + gram(i, abs(j - 1))) for j in range(n)] for i in range(n)]
    zero = jnp.zeros_like(m[0])

    def quad(a, Q):
        total = zero
        for i in range(len(a)):
            total = total + a[i] * a[i] * Q[i][i]
            for j in range(i):
                total = total + 2.0 * a[i] * a[j] * Q[i][j]
        return total

    def ratio(a, b):
        return jnp.where(b > 0.0, a / jnp.where(b > 0.0, b, 1.0), 0.0)

    z = [jnp.ones_like(zero)]
    p = list(z)
    x = [zero] * n
    rz = m[0]
    for it in range(n):
        alpha = ratio(rz, quad(p, H))
        for i in range(len(p)):
            x[i] = x[i] + alpha * p[i]
        if it + 1 == n:
            break
        image = p + [zero]
        for j in range(len(p)):
            if j == 0:
                image[1] = image[1] - p[0]
            else:
                image[j + 1] = image[j + 1] - 0.5 * p[j]
                image[j - 1] = image[j - 1] - 0.5 * p[j]
        z = [a - alpha * b for a, b in zip(z + [zero], image)]
        rz_next = quad(z, G)
        beta = ratio(rz_next, rz)
        p = [a + beta * b for a, b in zip(z, p + [zero])]
        rz = rz_next
    return x


def star_kernel(
    rows, total_rows, u, v, t, land, clinic, wet, edge, from_low, from_high, from_west, from_east,
    u_out, v_out, t_out,
):
    col_dev, row_dev = place()
    levels = u.shape[0]
    half = rows // 2
    below = {}
    for i, ref in enumerate((u, v, t)):
        for k in range(levels):
            n = SUB * NP + i * levels + k
            below[i, k] = from_low[n : n + 1, :]
    for r in range(0, rows, BY):
        block = row_dev * (rows // BY) + r // BY
        active = clinic[col_dev, block].astype(f32)
        here = slice(r, r + BY)
        keep = land[here, :].astype(f32) * active
        rest = 1.0 - active
        h = wet[here, :]
        lane = lane_of(h)
        first, last = lane == 0, lane == LANES - 1
        beside = edge[here, :]
        fe = jnp.minimum(h, jnp.where(last, roll(beside, LANES - 1 - SUB), roll(h, -1)))
        fw = jnp.minimum(h, jnp.where(first, roll(beside, -(SUB + 1)), roll(h, 1)))
        h_n = wet[r + 1 : r + BY + 1, :] if r + BY < rows else jnp.concatenate(
            [h[1:], edge[rows + SUB - 2 : rows + SUB - 1, :]], 0
        )
        h_s = wet[r - 1 : r + BY - 1, :] if r > 0 else jnp.concatenate(
            [edge[rows + SUB - 1 :, :], h[:-1]], 0
        )
        fn, fs = jnp.minimum(h, h_n), jnp.minimum(h, h_s)
        row = row_dev * rows + r + lax.broadcasted_iota(jnp.int32, (BY, LANES), 0)
        coriolis = 0.2 + 0.6 * ((row.astype(f32) + 0.5) / total_rows)
        src = slice(r % half, r % half + BY)
        base = HALF * (r // half) + EDGE
        now = {(i, k): ref[k, here, :] for i, ref in enumerate((u, v, t)) for k in range(levels)}

        def around(ref, which, k):
            i = SUB * NP + which * levels + k
            a = now[which, k]
            lo = base + which * levels + k
            e = jnp.where(last, roll(from_east[src, :], LANES - 1 - lo), roll(a, -1))
            w = jnp.where(first, roll(from_west[src, :], -lo), roll(a, 1))
            if r + BY < rows:
                n = ref[k, r + 1 : r + BY + 1, :]
            else:
                n = jnp.concatenate([a[1:], from_high[i : i + 1, :]], 0)
            s = jnp.concatenate([below[which, k], a[:-1]], 0)
            return a, e, w, n, s

        def diffuse(a, e, w, n, s):
            return fe * (e - a) + fw * (w - a) + fn * (n - a) + fs * (s - a)

        def mixing(which, k, a):
            total = None
            if k + 1 < levels:
                total = now[which, k + 1] - a
            if k > 0:
                down = a - now[which, k - 1]
                total = -down if total is None else total - down
            return jnp.zeros_like(a) if total is None else total

        results = []
        for k in range(levels):
            ua = around(u, 0, k)
            va = around(v, 1, k)
            ta = around(t, 2, k)
            uc, vc, tc = ua[0], va[0], ta[0]
            u_star = uc + step_time * (
                vertical * mixing(0, k, uc) + viscosity * diffuse(*ua) + coriolis * vc
            )
            v_star = vc + step_time * (
                vertical * mixing(1, k, vc) + viscosity * diffuse(*va) - coriolis * uc
            )
            raw = tc + step_time * (
                vertical * mixing(2, k, tc) + diffusivity * diffuse(*ta)
                - 0.5 * (uc * (ta[1] - ta[2]) + vc * (ta[3] - ta[4]))
            )
            t_out[k, here, :] = keep * raw + rest * tc
            results.append((keep * u_star + rest * uc, keep * v_star + rest * vc))
        below = {key: a[BY - 1 :] for key, a in now.items()}
        for k, (u_base, v_base) in enumerate(results):
            u_out[k, here, :] = u_base
            v_out[k, here, :] = v_base


def finish_kernel(
    rows, parts, basis, edge, land, clinic, u, v, u_out, v_out, p_out
):
    col_dev, row_dev = place()
    levels = u.shape[0]
    lane1 = lax.broadcasted_iota(jnp.int32, (1, LANES), 1)
    line = jnp.sum(parts[...], axis=0, keepdims=True)
    sums = []
    for i in range(2 * ITERS):
        one = jnp.sum(jnp.where(lane1 == i, line, 0.0), axis=1, keepdims=True)
        sums.append(jnp.broadcast_to(one, (1, LANES)))
    m = sums[:2] + [2.0 * s - sums[i % 2] for i, s in enumerate(sums[2:])]
    x = coefficients(m)
    weights = jnp.where(lane1 == 0, 1.0, 0.0)
    for k in range(ITERS):
        weights = jnp.where(lane1 == k + 1, x[k], weights)

    def mix(rows_of):
        total = rows_of(0)
        for k in range(ITERS):
            total = total + x[k] * rows_of(k + 1)
        return total

    for r in range(0, rows, BY):
        p_out[r : r + BY, :] = mix(lambda j: basis[j, r : r + BY, :])
    above = mix(lambda j: edge[rows + j : rows + j + 1, :])
    for r in range(0, rows, BY):
        here = slice(r, r + BY)
        p = p_out[here, :]
        active = clinic[col_dev, row_dev * (rows // BY) + r // BY].astype(f32)
        keep = land[here, :].astype(f32) * active
        side = jnp.sum(edge[here, :] * weights, axis=1, keepdims=True)
        east = jnp.where(lane_of(p) == LANES - 1, side, roll(p, -1))
        if r + BY < rows:
            north = p_out[r + 1 : r + BY + 1, :]
        else:
            north = jnp.concatenate([p[1:], above], 0)
        push_x = keep * (gravity * (east - p))
        push_y = keep * (gravity * (north - p))
        for k in range(levels):
            u_out[k, here, :] = u[k, here, :] - push_x
            v_out[k, here, :] = v[k, here, :] - push_y


VMEM = pl.BlockSpec(memory_space=pltpu.VMEM)
SMEM = pl.BlockSpec(memory_space=pltpu.SMEM)
ANY = pl.BlockSpec(memory_space=pl.ANY)
HBM = pl.BlockSpec(memory_space=pltpu.HBM)


def shape(*dims):
    return jax.ShapeDtypeStruct(dims, f32)


def on_device(
    velocity_u, velocity_v, tracer, pressure_old, depth, helm, land_mask, clinic_map, tropic_map
):
    levels, rows, cols = velocity_u.shape
    nx, ny = lax.axis_size("gx"), lax.axis_size("gy")
    total_rows = rows * ny
    assert cols == LANES == BX and rows % BY == 0 and rows % (2 * BY) == 0
    assert EDGE + 3 * levels <= HALF and ITERS + 2 <= SUB
    half = rows // 2
    ext = rows + 2 * SUB
    strip = -(-(SUB * NP + 3 * levels) // SUB) * SUB
    fields = (velocity_u, velocity_v, tracer, pressure_old, depth, helm, land_mask, tropic_map.T)

    def params(mib):
        return pltpu.CompilerParams(vmem_limit_bytes=mib << 20)

    low, high = pl.pallas_call(
        lambda *a: rim_kernel(rows, total_rows, *a),
        out_shape=(shape(strip, LANES), shape(strip, LANES)),
        in_specs=[HBM] * 7 + [SMEM],
        out_specs=(VMEM, VMEM),
        scratch_shapes=[
            pltpu.VMEM((2, 3, levels, SUB, LANES), f32),
            pltpu.VMEM((2, 3, SUB, LANES), f32),
            pltpu.VMEM((2, SUB, LANES), jnp.int32),
            pltpu.SemaphoreType.DMA((14,)),
        ],
        compiler_params=params(58),
        name="rim",
    )(*fields)
    up = [(i, (i + 1) % ny) for i in range(ny)]
    down = [((i + 1) % ny, i) for i in range(ny)]
    from_low = lax.ppermute(high, "gy", up)
    from_high = lax.ppermute(low, "gy", down)
    planes, wet, west, east, u_copy, v_copy = pl.pallas_call(
        lambda *a: plane_kernel(rows, total_rows, *a),
        out_shape=(
            shape(NP - 1, rows, LANES), shape(rows, LANES), shape(half + SUB, LANES),
            shape(half + SUB, LANES), shape(levels, rows, LANES), shape(levels, rows, LANES),
        ),
        in_specs=[VMEM] * 7 + [SMEM],
        out_specs=(VMEM,) * 6,
        compiler_params=params(6),
        name="planes",
    )(*fields)
    strip_spec = pl.BlockSpec((strip, LANES), lambda i: (0, 0))
    corner = pl.BlockSpec((SUB, LANES), lambda i: (half // SUB, 0))
    west, east = pl.pallas_call(
        corner_kernel,
        grid=(1,),
        out_shape=(shape(half + SUB, LANES),) * 2,
        in_specs=[strip_spec, strip_spec, ANY, ANY],
        out_specs=(corner, corner),
        input_output_aliases={2: 0, 3: 1},
        compiler_params=params(2),
        name="corners",
    )(from_low, from_high, west, east)
    right = [(i, (i + 1) % nx) for i in range(nx)]
    left = [((i + 1) % nx, i) for i in range(nx)]
    from_west = lax.ppermute(east, "gx", right)
    from_east = lax.ppermute(west, "gx", left)
    tall = ext + 2 * SUB
    basis, edge, partial = pl.pallas_call(
        lambda *a: solve_kernel(rows, *a),
        out_shape=(
            shape(ITERS + 1, rows, LANES), shape(rows + SUB, LANES),
            shape(nx * ny, LANES),
        ),
        in_specs=[VMEM] * 6,
        out_specs=(VMEM,) * 3,
        scratch_shapes=[
            pltpu.VMEM((NP, 2, tall, LANES), f32),
            pltpu.VMEM((2, tall, LANES), f32),
            pltpu.VMEM((2, tall, LANES), f32),
            pltpu.VMEM((2, tall, LANES), f32),
            pltpu.VMEM((2, tall, LANES), f32),
            pltpu.VMEM((ITERS, 2, tall, LANES), f32),
            pltpu.VMEM((4, 2, tall, LANES), f32),
            pltpu.VMEM((tall, LANES), f32),
        ],
        compiler_params=params(12),
        name="solve",
    )(planes, wet, from_low, from_high, from_west, from_east)
    parts = lax.all_to_all(partial, ("gx", "gy"), 0, 0, tiled=True)
    full = levels * rows * LANES
    u_base, v_base, t_new = pl.pallas_call(
        lambda *a: star_kernel(rows, total_rows, *a),
        out_shape=(shape(levels, rows, LANES),) * 3,
        in_specs=[VMEM] * 4 + [SMEM] + [VMEM] * 6,
        out_specs=(VMEM,) * 3,
        input_output_aliases={0: 0, 1: 1},
        compiler_params=params(8),
        cost_estimate=pl.CostEstimate(flops=400 * full, bytes_accessed=24 * full, transcendentals=0),
        name="star",
    )(
        u_copy, v_copy, tracer, land_mask, clinic_map.T, wet, edge, from_low, from_high,
        from_west, from_east,
    )
    u_new, v_new, pressure = pl.pallas_call(
        lambda *a: finish_kernel(rows, *a),
        out_shape=(shape(levels, rows, LANES),) * 2 + (shape(rows, LANES),),
        in_specs=[VMEM] * 4 + [SMEM] + [VMEM] * 2,
        out_specs=(VMEM,) * 3,
        compiler_params=params(4),
        name="finish",
    )(parts, basis, edge, land_mask, clinic_map.T, u_base, v_base)
    return u_new, v_new, t_new, pressure


def solution(mesh):
    in_specs = (
        P(None, "gy", "gx"),
        P(None, "gy", "gx"),
        P(None, "gy", "gx"),
        P("gy", "gx"),
        P("gy", "gx"),
        P("gy", "gx"),
        P("gy", "gx"),
        P(),
        P(),
    )
    out_specs = (P(None, "gy", "gx"), P(None, "gy", "gx"), P(None, "gy", "gx"), P("gy", "gx"))
    return jax.shard_map(
        on_device, mesh=mesh, in_specs=in_specs, out_specs=out_specs, check_vma=False
    )
```

```python
import jax
import jax.numpy as jnp
from jax import lax
from jax.experimental import pallas as pl
from jax.experimental.pallas import tpu as pltpu
from jax.sharding import PartitionSpec as P

BX = 128
BY = 40
ITERS = 4

step_time = 0.2
viscosity = 0.5
diffusivity = 0.5
vertical = 0.5
gravity = 1.0

SUB = 8
LANES = 128
HALF = LANES // 2
PLANES = ("U", "G", "V", "H", "wet", "start", "helm")
WIDTHS = (ITERS + 2, ITERS + 1, ITERS + 1, ITERS, ITERS + 2, ITERS + 1, ITERS)
OFFSETS = tuple(sum(WIDTHS[:i]) for i in range(len(WIDTHS)))
EDGE = sum(WIDTHS)
NP = len(PLANES)
WET = PLANES.index("wet")
OTHERS = tuple(i for i in range(NP) if i != WET)
f32 = jnp.float32


def roll(x, shift, axis=1):
    shift = shift % x.shape[axis]
    return x if shift == 0 else pltpu.roll(x, shift, axis)


def lane_of(x):
    return lax.broadcasted_iota(jnp.int32, x.shape, 1)


def thickness(levels):
    return [(2 * k + 1) / (levels * levels) for k in range(levels)]


def mixed_weights(levels):
    thick = thickness(levels)
    out = list(thick)
    for k in range(levels - 1):
        move = step_time * vertical * (thick[k] - thick[k + 1])
        out[k + 1] += move
        out[k] -= move
    return out


def weighted(weights, fields):
    total = weights[0] * fields[0]
    for w, f in zip(weights[1:], fields[1:]):
        total = total + w * f
    return total


def planes_of(us, vs, pressure_old, depth, helm, land, domain, first_row, total_rows):
    levels = len(us)
    thick, mixed = thickness(levels), mixed_weights(levels)
    row = first_row + lax.broadcasted_iota(jnp.int32, us[0].shape, 0)
    coriolis = 0.2 + 0.6 * ((row.astype(f32) + 0.5) / total_rows)
    u_sum, v_sum = weighted(thick, us), weighted(thick, vs)
    east = weighted(mixed, us) + step_time * coriolis * v_sum
    north = weighted(mixed, vs) - step_time * coriolis * u_sum
    mask = land.astype(f32) * domain
    return (u_sum, east, v_sum, north, depth * mask, mask * pressure_old, helm)


def place():
    return lax.axis_index("gx"), lax.axis_index("gy")


def pick(axis, a, b):
    odd = jnp.broadcast_to(lax.axis_index(axis) % 2, a.shape)
    return jnp.where(odd == 0, a, b)


def domain_at(tropic_ref, row_dev, col_dev, rows, row):
    block = row_dev * (rows // BY) + row // BY
    return jnp.where(tropic_ref[col_dev, block] >= 0, 1.0, 0.0).astype(f32)


def rim_kernel(
    rows, total_rows, u, v, t, p, depth, helm, land, tropic, near_out, far_out, s3, s2, si, sems
):
    col_dev, row_dev = place()
    levels = u.shape[0]
    copies = []
    for side, r0 in enumerate((0, rows - SUB)):
        for i, ref in enumerate((u, v, t)):
            copies.append((ref.at[:, pl.ds(r0, SUB), :], s3.at[side, i]))
        for i, ref in enumerate((p, depth, helm)):
            copies.append((ref.at[pl.ds(r0, SUB), :], s2.at[side, i]))
        copies.append((land.at[pl.ds(r0, SUB), :], si.at[side]))
    copies = [pltpu.make_async_copy(a, b, sems.at[i]) for i, (a, b) in enumerate(copies)]
    for c in copies:
        c.start()
    for c in copies:
        c.wait()
    strips = []
    for side, r0 in enumerate((0, rows - SUB)):
        domain = domain_at(tropic, row_dev, col_dev, rows, r0)
        us = [s3[side, 0, k] for k in range(levels)]
        vs = [s3[side, 1, k] for k in range(levels)]
        planes = planes_of(
            us, vs, s2[side, 0], s2[side, 1], s2[side, 2], si[side], domain,
            row_dev * rows + r0, total_rows,
        )
        edge = 0 if side == 0 else SUB - 1
        lines = [s3[side, i, k, edge : edge + 1, :] for i in range(3) for k in range(levels)]
        spare = near_out.shape[0] - SUB * NP - len(lines)
        lines.append(jnp.zeros((spare, LANES), f32))
        strips.append(list(planes) + [jnp.concatenate(lines, 0)])
    row = 0
    for low, high in zip(*strips):
        here = slice(row, row + low.shape[0])
        near_out[here, :] = pick("gy", high, low)
        far_out[here, :] = pick("gy", low, high)
        row += low.shape[0]


def pack_pair(low_fields, high_fields, extra_low, extra_high, to_west):
    shape = low_fields[0].shape
    lane = lax.broadcasted_iota(jnp.int32, shape, 1)
    out = jnp.zeros(shape, f32)
    for base, fields, extra in ((0, low_fields, extra_low), (HALF, high_fields, extra_high)):
        for f, w, off in zip(fields, WIDTHS, OFFSETS):
            lo = base + off
            first = 0 if to_west else LANES - w
            out = jnp.where((lane >= lo) & (lane < lo + w), roll(f, lo - first), out)
        for i, f in enumerate(extra):
            lo = base + EDGE + i
            first = 0 if to_west else LANES - 1
            out = jnp.where(lane == lo, roll(f, lo - first), out)
    return out


def plane_kernel(
    rows, total_rows, u, v, t, p, depth, helm, land, tropic, clinic, planes, wet, state, near, far,
    u_copy, v_copy
):
    col_dev, row_dev = place()
    levels = u.shape[0]
    half = rows // 2

    def at(r):
        r = pl.multiple_of(r, SUB)
        here = pl.ds(r, SUB)
        us = [u[k, here, :] for k in range(levels)]
        vs = [v[k, here, :] for k in range(levels)]
        ts = [t[k, here, :] for k in range(levels)]
        domain = domain_at(tropic, row_dev, col_dev, rows, r)
        out = planes_of(
            us, vs, p[here, :], depth[here, :], helm[here, :], land[here, :], domain,
            row_dev * rows + r, total_rows,
        )
        for i, plane in zip(OTHERS, range(NP - 1)):
            planes[plane, here, :] = out[i]
        wet[here, :] = out[WET]
        block = row_dev * (rows // BY) + r // BY
        active = clinic[col_dev, block].astype(f32)
        state[here, :] = active + active * land[here, :].astype(f32)
        for k in range(levels):
            u_copy[k, here, :] = us[k]
            v_copy[k, here, :] = vs[k]
        return out, us + vs + ts

    unroll = 4

    def body(i, carry):
        for j in range(unroll):
            r = (i * unroll + j) * SUB
            low, extra_low = at(r)
            high, extra_high = at(r + half)
            here = pl.ds(pl.multiple_of(r, SUB), SUB)
            west = pack_pair(low, high, extra_low, extra_high, True)
            east = pack_pair(low, high, extra_low, extra_high, False)
            near[here, :] = pick("gx", east, west)
            far[here, :] = pick("gx", west, east)
        return carry

    lax.fori_loop(0, half // (SUB * unroll), body, 0)


def corner_kernel(near_row, far_row, near_in, far_in, near, far):
    low, high = [], []
    for i in range(NP):
        here = slice(SUB * i, SUB * i + SUB)
        a, b = near_row[here, :], far_row[here, :]
        low.append(pick("gy", b, a))
        high.append(pick("gy", a, b))
    west = pack_pair(low, high, [], [], True)
    east = pack_pair(low, high, [], [], False)
    near[...] = pick("gx", east, west)
    far[...] = pick("gx", west, east)


def shifted(c, h):
    lane = lane_of(c)
    rc, rh = roll(c, -1), roll(h, -1)
    last = lane == LANES - 1
    east = jnp.where(last, rh, rc), jnp.where(last, rc, rh)
    rc, rh = roll(c, 1), roll(h, 1)
    first = lane == 0
    west = jnp.where(first, rh, rc), jnp.where(first, rc, rh)
    return east, west


CH = 24


def solve_kernel(
    rows, planes, wet_in, near_row, far_row, near_col, far_col,
    basis, edge, partial, F, face_e, face_n, flow_e, flow_n, T, coef, diag,
):
    ext = rows + 2 * SUB
    half = rows // 2
    top = ext + SUB
    zero8 = jnp.zeros((SUB, LANES), f32)
    for c in range(2):
        for r in (0, top):
            for i in range(NP):
                F[i, c, pl.ds(r, SUB), :] = zero8
            face_e[c, pl.ds(r, SUB), :] = zero8
            face_n[c, pl.ds(r, SUB), :] = zero8
            flow_n[c, pl.ds(r, SUB), :] = zero8
            for k in range(ITERS):
                T[k, c, pl.ds(r, SUB), :] = zero8

    def unpack(dst, src, base):
        a, b = near_col[src, :], far_col[src, :]
        e, w = pick("gx", a, b), pick("gx", b, a)
        lane = lane_of(e)
        for i in range(NP):
            lo = base + OFFSETS[i]
            width = WIDTHS[i]
            he = roll(e, -lo)
            hw = roll(w, LANES - width - lo)
            h = jnp.where(lane < width, he, jnp.where(lane >= LANES - width, hw, 0.0))
            F[i, 1, dst, :] = h

    for i in range(NP):
        a, b = near_row[pl.ds(SUB * i, SUB), :], far_row[pl.ds(SUB * i, SUB), :]
        F[i, 0, pl.ds(SUB, SUB), :] = pick("gy", b, a)
        F[i, 0, pl.ds(SUB + SUB + rows, SUB), :] = pick("gy", a, b)
        F[i, 0, pl.ds(2 * SUB, rows), :] = wet_in[...] if i == WET else planes[OTHERS.index(i)]
    unpack(pl.ds(SUB, SUB), pl.ds(half, SUB), 0)
    unpack(pl.ds(2 * SUB + rows, SUB), pl.ds(half, SUB), HALF)
    step = 40
    for r in range(0, half, step):
        unpack(pl.ds(2 * SUB + r, step), pl.ds(r, step), 0)
        unpack(pl.ds(2 * SUB + half + r, step), pl.ds(r, step), HALF)

    iU, iG, iV, iH, iW, iS, iM = range(NP)
    chunks = [(SUB + r) for r in range(0, ext, CH)]
    assert ext % CH == 0
    both = (0, 1)

    def load(ref, idx, r, d=0):
        return tuple(ref[idx + (c, slice(r + d, r + d + CH), slice(None))] for c in both)

    def store(ref, idx, r, value):
        for c in both:
            ref[idx + (c, slice(r, r + CH), slice(None))] = value[c]

    def around(ref, idx, r):
        x = load(ref, idx, r)
        e, w = shifted(*x)
        return x, e, w, load(ref, idx, r, 1), load(ref, idx, r, -1)

    def stage_faces(r):
        x, e, _, n, _ = around(F, (iW,), r)
        store(face_e, (), r, tuple(jnp.minimum(x[c], e[c]) for c in both))
        store(face_n, (), r, tuple(jnp.minimum(x[c], n[c]) for c in both))

    def stage_flows(r):
        fe, fn, fs = load(face_e, (), r), load(face_n, (), r), load(face_n, (), r, -1)
        _, fw = shifted(*fe)
        wet = load(F, (iW,), r)
        for field, base, out in ((iU, iG, flow_e), (iV, iH, flow_n)):
            x, e, w, n, s = around(F, (field,), r)
            g = load(F, (base,), r)
            flow = []
            for c in both:
                d = (
                    fe[c] * (e[c] - x[c]) + fw[c] * (w[c] - x[c])
                    + fn[c] * (n[c] - x[c]) + fs[c] * (s[c] - x[c])
                )
                flow.append(wet[c] * (g[c] + (step_time * viscosity) * d))
            store(out, (), r, flow)

    def core_rows(r):
        lo, hi = max(r, 2 * SUB), min(r + CH, 2 * SUB + rows)
        return lo - r, hi - r

    def keep_core(ref, i, r, value):
        lo, hi = core_rows(r)
        ref[i, r + lo - 2 * SUB : r + hi - 2 * SUB, :] = value[lo:hi]

    sums = [None] * (2 * ITERS)

    def add_sum(i, r, value):
        lo, hi = core_rows(r)
        for q in range(lo, hi, SUB):
            part = value[q : q + SUB]
            sums[i] = part if sums[i] is None else sums[i] + part

    def stage_residual(r):
        fe, fn, fs = load(face_e, (), r), load(face_n, (), r), load(face_n, (), r, -1)
        _, fw = shifted(*fe)
        wet, helm = load(F, (iW,), r), load(F, (iM,), r)
        ef = load(flow_e, (), r)
        _, efw = shifted(*ef)
        nf, nfs = load(flow_n, (), r), load(flow_n, (), r, -1)
        x, e, w, n, s = around(F, (iS,), r)
        for c in both:
            mask = wet[c] > 0.0
            force = jnp.where(mask, -(ef[c] - efw[c]) - (nf[c] - nfs[c]), 0.0)
            d = helm[c] + fe[c] + fw[c] + fn[c] + fs[c]
            res = force - (
                d * x[c] - fe[c] * e[c] - fw[c] * w[c] - fn[c] * n[c] - fs[c] * s[c]
            )
            inv = 1.0 / jnp.where(d > 0.0, d, 1.0)
            z = res * inv
            here = slice(r, r + CH)
            T[0, c, here, :] = z
            for i, f in enumerate((fe, fw, fn, fs)):
                coef[i, c, here, :] = f[c] * inv
            if c == 0:
                diag[here, :] = d
                add_sum(0, r, res * z)
                keep_core(basis, 0, r, x[0])
                keep_core(basis, 1, r, z)

    def stage_step(k, r):
        x, e, w, n, s = around(T, (k,), r)
        here = slice(r, r + CH)
        for c in both if k + 1 < ITERS else (0,):
            y = (
                coef[0, c, here, :] * e[c] + coef[1, c, here, :] * w[c]
                + coef[2, c, here, :] * n[c] + coef[3, c, here, :] * s[c]
            )
            if k > 0:
                y = 2.0 * y - T[k - 1, c, here, :]
            if k + 1 < ITERS:
                T[k + 1, c, here, :] = y
            if c == 0:
                d = diag[here, :]
                add_sum(2 * k + 1, r, d * x[c] * y)
                if k + 1 < ITERS:
                    add_sum(2 * k + 2, r, d * y * y)
                    keep_core(basis, k + 2, r, y)

    stages = [stage_faces, stage_flows, stage_residual]
    stages += [lambda r, k=k: stage_step(k, r) for k in range(ITERS)]
    lags = [0]
    for _ in stages[1:]:
        lags.append(lags[-1] + 1)
    lags = [0, 1, 2] + [2 + 2 * (k + 1) for k in range(ITERS)]
    for i in range(len(chunks) + lags[-1]):
        for stage, lag in zip(stages, lags):
            if 0 <= i - lag < len(chunks):
                stage(chunks[i - lag])

    vectors = [lambda c, here: F[iS, c, here, :]]
    vectors += [lambda c, here, k=k: T[k, c, here, :] for k in range(ITERS)]
    assert len(vectors) + 2 <= SUB
    for r in range(0, rows, BY):
        here = slice(2 * SUB + r, 2 * SUB + r + BY)
        side = F[iW, 1, here, :]
        lane = lane_of(side)
        tile = jnp.where(lane == SUB, roll(side, SUB), 0.0)
        tile = jnp.where(lane == SUB + 1, roll(side, SUB + 2), tile)
        for j, get in enumerate(vectors):
            tile = jnp.where(lane == j, roll(get(1, here), j), tile)
        edge[r : r + BY, :] = tile
    north = 2 * SUB + rows
    edge[rows:, :] = jnp.zeros((SUB, LANES), f32)
    for j, get in enumerate(vectors):
        edge[rows + j : rows + j + 1, :] = get(0, slice(north, north + 1))
    edge[rows + SUB - 2 : rows + SUB - 1, :] = F[iW, 0, north : north + 1, :]
    edge[rows + SUB - 1 :, :] = F[iW, 0, 2 * SUB - 1 : 2 * SUB, :]
    lane = lax.broadcasted_iota(jnp.int32, (1, LANES), 1)
    line = jnp.zeros((1, LANES), f32)
    for i, total in enumerate(sums):
        one = jnp.sum(jnp.sum(total, axis=0, keepdims=True), axis=1, keepdims=True)
        line = jnp.where(lane == i, one, line)
    partial[...] = jnp.broadcast_to(line, partial.shape)


def coefficients(m):
    n = ITERS

    def gram(i, j):
        return 0.5 * (m[i + j] + m[abs(i - j)])

    G = [[gram(i, j) for j in range(n)] for i in range(n)]
    H = [[gram(i, j) - 0.5 * (gram(i, j + 1) + gram(i, abs(j - 1))) for j in range(n)] for i in range(n)]
    zero = jnp.zeros_like(m[0])

    def quad(a, Q):
        total = zero
        for i in range(len(a)):
            total = total + a[i] * a[i] * Q[i][i]
            for j in range(i):
                total = total + 2.0 * a[i] * a[j] * Q[i][j]
        return total

    def ratio(a, b):
        return jnp.where(b > 0.0, a / jnp.where(b > 0.0, b, 1.0), 0.0)

    z = [jnp.ones_like(zero)]
    p = list(z)
    x = [zero] * n
    rz = m[0]
    for it in range(n):
        alpha = ratio(rz, quad(p, H))
        for i in range(len(p)):
            x[i] = x[i] + alpha * p[i]
        if it + 1 == n:
            break
        image = p + [zero]
        for j in range(len(p)):
            if j == 0:
                image[1] = image[1] - p[0]
            else:
                image[j + 1] = image[j + 1] - 0.5 * p[j]
                image[j - 1] = image[j - 1] - 0.5 * p[j]
        z = [a - alpha * b for a, b in zip(z + [zero], image)]
        rz_next = quad(z, G)
        beta = ratio(rz_next, rz)
        p = [a + beta * b for a, b in zip(z, p + [zero])]
        rz = rz_next
    return x


def star_kernel(
    rows, total_rows, u, v, t, state, wet, edge, near_row, far_row, near_col, far_col,
    u_out, v_out, t_out,
):
    col_dev, row_dev = place()
    levels = u.shape[0]
    half = rows // 2
    below = {}
    for i, ref in enumerate((u, v, t)):
        for k in range(levels):
            n = SUB * NP + i * levels + k
            below[i, k] = pick("gy", far_row[n : n + 1, :], near_row[n : n + 1, :])
    for r in range(0, rows, BY):
        here = slice(r, r + BY)
        kind = state[here, :]
        keep = jnp.where(kind > 1.5, 1.0, 0.0)
        rest = jnp.where(kind < 0.5, 1.0, 0.0)
        h = wet[here, :]
        lane = lane_of(h)
        first, last = lane == 0, lane == LANES - 1
        beside = edge[here, :]
        fe = jnp.minimum(h, jnp.where(last, roll(beside, LANES - 1 - SUB), roll(h, -1)))
        fw = jnp.minimum(h, jnp.where(first, roll(beside, -(SUB + 1)), roll(h, 1)))
        h_n = wet[r + 1 : r + BY + 1, :] if r + BY < rows else jnp.concatenate(
            [h[1:], edge[rows + SUB - 2 : rows + SUB - 1, :]], 0
        )
        h_s = wet[r - 1 : r + BY - 1, :] if r > 0 else jnp.concatenate(
            [edge[rows + SUB - 1 :, :], h[:-1]], 0
        )
        fn, fs = jnp.minimum(h, h_n), jnp.minimum(h, h_s)
        row = row_dev * rows + r + lax.broadcasted_iota(jnp.int32, (BY, LANES), 0)
        coriolis = 0.2 + 0.6 * ((row.astype(f32) + 0.5) / total_rows)
        src = slice(r % half, r % half + BY)
        base = HALF * (r // half) + EDGE
        a, b = near_col[src, :], far_col[src, :]
        from_east, from_west = pick("gx", a, b), pick("gx", b, a)
        now = {(i, k): ref[k, here, :] for i, ref in enumerate((u, v, t)) for k in range(levels)}

        def around(ref, which, k):
            i = SUB * NP + which * levels + k
            a = now[which, k]
            lo = base + which * levels + k
            e = jnp.where(last, roll(from_east, LANES - 1 - lo), roll(a, -1))
            w = jnp.where(first, roll(from_west, -lo), roll(a, 1))
            if r + BY < rows:
                n = ref[k, r + 1 : r + BY + 1, :]
            else:
                above = pick("gy", near_row[i : i + 1, :], far_row[i : i + 1, :])
                n = jnp.concatenate([a[1:], above], 0)
            s = jnp.concatenate([below[which, k], a[:-1]], 0)
            return a, e, w, n, s

        def diffuse(a, e, w, n, s):
            return fe * (e - a) + fw * (w - a) + fn * (n - a) + fs * (s - a)

        def mixing(which, k, a):
            total = None
            if k + 1 < levels:
                total = now[which, k + 1] - a
            if k > 0:
                down = a - now[which, k - 1]
                total = -down if total is None else total - down
            return jnp.zeros_like(a) if total is None else total

        results = []
        for k in range(levels):
            ua = around(u, 0, k)
            va = around(v, 1, k)
            ta = around(t, 2, k)
            uc, vc, tc = ua[0], va[0], ta[0]
            u_star = uc + step_time * (
                vertical * mixing(0, k, uc) + viscosity * diffuse(*ua) + coriolis * vc
            )
            v_star = vc + step_time * (
                vertical * mixing(1, k, vc) + viscosity * diffuse(*va) - coriolis * uc
            )
            raw = tc + step_time * (
                vertical * mixing(2, k, tc) + diffusivity * diffuse(*ta)
                - 0.5 * (uc * (ta[1] - ta[2]) + vc * (ta[3] - ta[4]))
            )
            t_out[k, here, :] = keep * raw + rest * tc
            results.append((keep * u_star + rest * uc, keep * v_star + rest * vc))
        below = {key: a[BY - 1 :] for key, a in now.items()}
        for k, (u_base, v_base) in enumerate(results):
            u_out[k, here, :] = u_base
            v_out[k, here, :] = v_base


def finish_kernel(
    rows, parts, basis, edge, state, u, v, u_out, v_out, p_out
):
    levels = u.shape[0]
    lane1 = lax.broadcasted_iota(jnp.int32, (1, LANES), 1)
    line = jnp.sum(parts[...], axis=0, keepdims=True)
    sums = []
    for i in range(2 * ITERS):
        one = jnp.sum(jnp.where(lane1 == i, line, 0.0), axis=1, keepdims=True)
        sums.append(jnp.broadcast_to(one, (1, LANES)))
    m = sums[:2] + [2.0 * s - sums[i % 2] for i, s in enumerate(sums[2:])]
    x = coefficients(m)
    weights = jnp.where(lane1 == 0, 1.0, 0.0)
    for k in range(ITERS):
        weights = jnp.where(lane1 == k + 1, x[k], weights)

    def mix(rows_of):
        total = rows_of(0)
        for k in range(ITERS):
            total = total + x[k] * rows_of(k + 1)
        return total

    for r in range(0, rows, BY):
        p_out[r : r + BY, :] = mix(lambda j: basis[j, r : r + BY, :])
    above = mix(lambda j: edge[rows + j : rows + j + 1, :])
    for r in range(0, rows, BY):
        here = slice(r, r + BY)
        p = p_out[here, :]
        keep = jnp.where(state[here, :] > 1.5, 1.0, 0.0)
        side = jnp.sum(edge[here, :] * weights, axis=1, keepdims=True)
        east = jnp.where(lane_of(p) == LANES - 1, side, roll(p, -1))
        if r + BY < rows:
            north = p_out[r + 1 : r + BY + 1, :]
        else:
            north = jnp.concatenate([p[1:], above], 0)
        push_x = keep * (gravity * (east - p))
        push_y = keep * (gravity * (north - p))
        for k in range(levels):
            u_out[k, here, :] = u[k, here, :] - push_x
            v_out[k, here, :] = v[k, here, :] - push_y


VMEM = pl.BlockSpec(memory_space=pltpu.VMEM)
SMEM = pl.BlockSpec(memory_space=pltpu.SMEM)
ANY = pl.BlockSpec(memory_space=pl.ANY)
HBM = pl.BlockSpec(memory_space=pltpu.HBM)


def shape(*dims):
    return jax.ShapeDtypeStruct(dims, f32)


def exchange(near, far, axis):
    n = lax.axis_size(axis)
    far = lax.ppermute(far, axis, [(i, (i + (1 if i % 2 else -1)) % n) for i in range(n)])
    near = lax.ppermute(near, axis, [(i, i ^ 1) for i in range(n)])
    return near, far


def on_device(
    velocity_u, velocity_v, tracer, pressure_old, depth, helm, land_mask, clinic_map, tropic_map
):
    levels, rows, cols = velocity_u.shape
    nx, ny = lax.axis_size("gx"), lax.axis_size("gy")
    total_rows = rows * ny
    assert cols == LANES == BX and rows % BY == 0 and rows % (2 * BY) == 0
    assert nx % 2 == 0 and ny % 2 == 0
    assert EDGE + 3 * levels <= HALF and ITERS + 2 <= SUB
    half = rows // 2
    ext = rows + 2 * SUB
    strip = -(-(SUB * NP + 3 * levels) // SUB) * SUB
    fields = (velocity_u, velocity_v, tracer, pressure_old, depth, helm, land_mask, tropic_map.T)

    def params(mib):
        return pltpu.CompilerParams(vmem_limit_bytes=mib << 20)

    pinned = [pltpu.with_memory_space_constraint(f, pltpu.HBM) for f in fields[:7]]
    near, far = pl.pallas_call(
        lambda *a: rim_kernel(rows, total_rows, *a),
        out_shape=(shape(strip, LANES), shape(strip, LANES)),
        in_specs=[HBM] * 7 + [SMEM],
        out_specs=(VMEM, VMEM),
        scratch_shapes=[
            pltpu.VMEM((2, 3, levels, SUB, LANES), f32),
            pltpu.VMEM((2, 3, SUB, LANES), f32),
            pltpu.VMEM((2, SUB, LANES), jnp.int32),
            pltpu.SemaphoreType.DMA((14,)),
        ],
        compiler_params=params(2),
        name="rim",
    )(*pinned, pltpu.with_memory_space_constraint(tropic_map.T, pltpu.HBM))
    near_row, far_row = exchange(near, far, "gy")
    planes, wet, state, near, far, u_copy, v_copy = pl.pallas_call(
        lambda *a: plane_kernel(rows, total_rows, *a),
        out_shape=(
            shape(NP - 1, rows, LANES), shape(rows, LANES), shape(rows, LANES),
            shape(half + SUB, LANES),
            shape(half + SUB, LANES), shape(levels, rows, LANES), shape(levels, rows, LANES),
        ),
        in_specs=[VMEM] * 7 + [SMEM] * 2,
        out_specs=(VMEM,) * 7,
        compiler_params=params(6),
        name="planes",
    )(*fields, clinic_map.T)
    strip_spec = pl.BlockSpec((strip, LANES), lambda i: (0, 0))
    corner = pl.BlockSpec((SUB, LANES), lambda i: (half // SUB, 0))
    near, far = pl.pallas_call(
        corner_kernel,
        grid=(1,),
        out_shape=(shape(half + SUB, LANES),) * 2,
        in_specs=[strip_spec, strip_spec, ANY, ANY],
        out_specs=(corner, corner),
        input_output_aliases={2: 0, 3: 1},
        compiler_params=params(2),
        name="corners",
    )(near_row, far_row, near, far)
    near_col, far_col = exchange(near, far, "gx")
    tall = ext + 2 * SUB
    basis, edge, partial = pl.pallas_call(
        lambda *a: solve_kernel(rows, *a),
        out_shape=(
            shape(ITERS + 1, rows, LANES), shape(rows + SUB, LANES),
            shape(nx * ny, LANES),
        ),
        in_specs=[VMEM] * 6,
        out_specs=(VMEM,) * 3,
        scratch_shapes=[
            pltpu.VMEM((NP, 2, tall, LANES), f32),
            pltpu.VMEM((2, tall, LANES), f32),
            pltpu.VMEM((2, tall, LANES), f32),
            pltpu.VMEM((2, tall, LANES), f32),
            pltpu.VMEM((2, tall, LANES), f32),
            pltpu.VMEM((ITERS, 2, tall, LANES), f32),
            pltpu.VMEM((4, 2, tall, LANES), f32),
            pltpu.VMEM((tall, LANES), f32),
        ],
        compiler_params=params(12),
        name="solve",
    )(planes, wet, near_row, far_row, near_col, far_col)
    parts = lax.all_to_all(partial, ("gx", "gy"), 0, 0, tiled=True)
    full = levels * rows * LANES
    u_base, v_base, t_new = pl.pallas_call(
        lambda *a: star_kernel(rows, total_rows, *a),
        out_shape=(shape(levels, rows, LANES),) * 3,
        in_specs=[VMEM] * 10,
        out_specs=(VMEM,) * 3,
        input_output_aliases={0: 0, 1: 1},
        compiler_params=params(8),
        cost_estimate=pl.CostEstimate(flops=400 * full, bytes_accessed=24 * full, transcendentals=0),
        name="star",
    )(
        u_copy, v_copy, tracer, state, wet, edge, near_row, far_row, near_col, far_col
    )
    u_new, v_new, pressure = pl.pallas_call(
        lambda *a: finish_kernel(rows, *a),
        out_shape=(shape(levels, rows, LANES),) * 2 + (shape(rows, LANES),),
        in_specs=[VMEM] * 6,
        out_specs=(VMEM,) * 3,
        compiler_params=params(4),
        name="finish",
    )(parts, basis, edge, state, u_base, v_base)
    return u_new, v_new, t_new, pressure


def solution(mesh):
    in_specs = (
        P(None, "gy", "gx"),
        P(None, "gy", "gx"),
        P(None, "gy", "gx"),
        P("gy", "gx"),
        P("gy", "gx"),
        P("gy", "gx"),
        P("gy", "gx"),
        P(),
        P(),
    )
    out_specs = (P(None, "gy", "gx"), P(None, "gy", "gx"), P(None, "gy", "gx"), P("gy", "gx"))
    return jax.shard_map(
        on_device, mesh=mesh, in_specs=in_specs, out_specs=out_specs, check_vma=False
    )
```
